256 devices in a mesh: groups: 2 (over y), seq: 128 (over x, z, core).
Axes of the slice: x: 4, y: 2, z: 16, core: 2. Of those that a mesh axis runs over, the one named last changes fastest.
The devices are a block of a 4x16x16 slice.
Arguments:
- hidden: bfloat16 [8192, 3584], P(('groups', 'seq')), parts along dimension 0, may hold values from -6 to 6
- norm_gain: float32 [3584], replicated, may hold values from -0.5 to 0.5
- kv_weight: bfloat16 [28672, 512], P('seq'), may hold values from -0.09375 to 0.09375
- queries: bfloat16 [32, 16, 256], P('groups'), parts along dimension 0, may hold values from -300 to 300
- page_seqs: int32 [4096], P('groups'), parts along dimension 0, may hold values from 0 to 15, as said below
- page_slots: int32 [4096], P('groups'), parts along dimension 0, may hold values from 0 to 127, as said below
- lengths: int32 [32], P('groups'), parts along dimension 0, may hold values from 1 to 256
Outputs:
- attended: bfloat16 [32, 4096], P('groups', 'seq'), parts along dimension 0
The draws below stay inside these ranges and needn't reach their ends.
There are 2 independent parts, one for each index of `groups`. The reference program is written for one: setup_inputs(seed, part) draws one part's arguments, and reference() takes and returns one part's arrays. A program takes and returns all parts, laid end to end along the dimension named above; an argument that names none is the same for every part. Nothing has to cross between parts.
Inputs may be any that keep to these rules, and one draw needn't show every extreme that they name: `page_seqs`: every sequence owns exactly 128 pages. `page_slots`: the pages of one sequence carry the places 0 to 127, each once.
All inputs are finite; a program needn't handle non-finite values.
Results may differ from the reference program's by a relative error of at most 0.012.
The reference program's roundings to bfloat16 on the way (of `normed`, `keys` and `values`) count: a program that leaves them out, or rounds other values in their place, can miss the bound.
Values may be sent and summed in bfloat16 or wider, within the bound.
No kernel may reach another device: no remote copies, remote signals or barrier semaphores. Data moves between devices by JAX's collectives and lax.ppermute only.
A program may use at most 64 MiB of HBM per device.

```python
import jax
import jax.numpy as jnp
from jax import lax

D = 3584
HEAD = 256
KVH = 8
QH = 16
SEQS = 16
PAGE = 2
TOKENS = 4096
PAGES = 2048
CAP_PAGES = 128
SEQ_CAP = 256


def table_draw(key):
    shuffled = jax.random.permutation(jax.random.fold_in(key, 11), PAGES).astype(jnp.int32)
    return (shuffled // CAP_PAGES, shuffled % CAP_PAGES)


def draw_page_seqs(key, part):
    return table_draw(key)[0]


def draw_page_slots(key, part):
    return table_draw(key)[1]


def draw_queries(key, part):
    base = jnp.clip(jax.random.normal(jax.random.fold_in(key, 23), (SEQS, QH, HEAD), jnp.float32), -4.0, 4.0) * 1.5
    return base.astype(jnp.bfloat16)


def with_ends(values, key, smallest, high):
    index_at = [jax.random.randint(jax.random.fold_in(key, axis), (), 0, length) for axis, length in enumerate(values.shape)]
    widest = values.shape.index(max(values.shape))
    neighbour = index_at[:widest] + [(index_at[widest] + 1) % values.shape[widest]] + index_at[widest + 1:]
    return values.at[tuple(index_at)].set(smallest).at[tuple(neighbour)].set(high)


def steps_of(key, dims, split, smallest, high):
    gain, own = 1.0, jax.random.fold_in(key, 6)
    for position, blocks in split:
        draws = jnp.exp(jax.random.uniform(jax.random.fold_in(own, position), (blocks,), jnp.float32, smallest / len(split), high / len(split)))
        gain = gain * jnp.repeat(draws, dims[position] // blocks).reshape([-1 if axis == position else 1 for axis in range(len(dims))])
    return gain


def scatter_about(stream_key, dims, scale, reach, cuts=(), kind=jnp.bfloat16):
    values = jax.random.normal(stream_key, dims, jnp.float32) * scale
    if len(cuts) > 0:
        values = steps_of(stream_key, dims, cuts, -0.22, 0.18) * values
    return jnp.clip(values, min=-reach, max=reach).astype(kind)


def setup_inputs(seed: int = 0, part: int = 0) -> dict:
    key_list = jax.random.split(jax.random.key(seed), 8)
    part_keys = jax.random.split(jax.random.fold_in(key_list[7], part), 8)
    hidden = scatter_about(part_keys[0], (TOKENS, D), 1.0, 6.0, ((0, 128),))
    norm_gain = jnp.clip(jax.random.uniform(key_list[1], (D,), jnp.float32, -0.5, 0.5), -0.5, 0.5)
    kv_weight = scatter_about(key_list[2], (KVH * D, 2 * HEAD), D ** -0.5, 0.09375, ((0, 128),))
    queries = draw_queries(jax.random.fold_in(jax.random.fold_in(key_list[7], part), 71), part)
    page_seqs = draw_page_seqs(jax.random.fold_in(jax.random.fold_in(key_list[7], part), 71), part)
    page_slots = draw_page_slots(jax.random.fold_in(jax.random.fold_in(key_list[7], part), 71), part)
    lengths = with_ends(jax.random.randint(part_keys[6], (SEQS,), 1, SEQ_CAP + 1), jax.random.fold_in(part_keys[6], 1), 1, SEQ_CAP).astype(jnp.int32)
    return dict(hidden=hidden, norm_gain=norm_gain, kv_weight=kv_weight, queries=queries, page_seqs=page_seqs, page_slots=page_slots, lengths=lengths)


def rotate(keys_raw, positions):
    half_dim = keys_raw.shape[-1] // 2
    inverse_freq = jnp.exp(-(2.0 * jnp.arange(half_dim, dtype=jnp.float32) / keys_raw.shape[-1]) * jnp.log(jnp.float32(10000.0)))
    angles = positions.astype(jnp.float32)[:, None] * inverse_freq[None, :]
    cosine = jnp.cos(angles)
    sine = jnp.sin(angles)
    first = keys_raw[:, :half_dim]
    second = keys_raw[:, half_dim:]
    return jnp.concatenate([first * cosine - second * sine, second * cosine + first * sine], axis=1)

def reference(hidden, norm_gain, kv_weight, queries, page_seqs, page_slots, lengths):
    token_ids = jnp.arange(TOKENS, dtype=jnp.int32)
    page_ids = token_ids // PAGE
    positions = page_slots[page_ids] * PAGE + token_ids % PAGE
    token_seqs = page_seqs[page_ids]
    valid = (token_seqs[None, :] == jnp.arange(SEQS, dtype=jnp.int32)[:, None]) & (positions[None, :] < lengths[:, None])
    wide = hidden.astype(jnp.float32)
    scale_rows = lax.rsqrt(lax.optimization_barrier(jnp.mean(wide * wide, axis=1, keepdims=True)) + 1e-06)
    normed = (wide * scale_rows * (1.0 + norm_gain)[None, :]).astype(jnp.bfloat16)
    weights_3d = kv_weight.reshape(KVH, D, 2 * HEAD)

    def one_head(head_index):
        weight_now = lax.dynamic_index_in_dim(weights_3d, head_index, 0, keepdims=False)
        projected = jnp.dot(normed, weight_now, preferred_element_type=jnp.float32)
        keys = rotate(projected[:, :HEAD], positions).astype(jnp.bfloat16)
        values = projected[:, HEAD:].astype(jnp.bfloat16)
        head_queries = lax.dynamic_slice_in_dim(queries, 2 * head_index, 2, 1).astype(jnp.float32)
        score = jnp.einsum('sjd,td->sjt', head_queries, keys.astype(jnp.float32), precision=lax.Precision.HIGHEST) * HEAD ** (-0.5)
        keep = valid[:, None, :]
        masked = jnp.where(keep, score, jnp.float32(-1e+30))
        row_max = lax.optimization_barrier(jnp.max(masked, axis=2, keepdims=True))
        probs = jnp.where(keep, jnp.exp(masked - row_max), jnp.float32(0.0))
        row_sum = lax.optimization_barrier(jnp.sum(probs, axis=2, keepdims=True))
        weighted = jnp.einsum('sjt,td->sjd', probs, values.astype(jnp.float32), precision=lax.Precision.HIGHEST)
        return weighted / row_sum
    per_head = lax.map(one_head, jnp.arange(KVH, dtype=jnp.int32))
    ordered = jnp.transpose(per_head, (1, 0, 2, 3)).reshape(SEQS, QH * HEAD)
    return ordered.astype(jnp.bfloat16)
```

```python
import functools

import jax
import jax.numpy as jnp
from jax import lax
from jax.experimental import pallas as pl
from jax.experimental.pallas import tpu as pltpu
from jax.sharding import PartitionSpec as P

HEAD = 256
KVH = 8
CORES = 2
RING = 16
HALF = RING // 2


VMEM = pl.BlockSpec(memory_space=pltpu.VMEM)
SMEM = pl.BlockSpec(memory_space=pltpu.SMEM)


def moves(n_devices, step):
    n_cols = n_devices // (RING * CORES)
    pairs = []
    for i in range(n_devices):
        col, row, core = i // (RING * CORES), i // CORES % RING, i % CORES
        col, row, core = step(col, row, core)
        pairs.append((i, (col % n_cols * RING + row % RING) * CORES + core))
    return pairs


def project(where_ref, x_ref, acc_ref, pieces, first):
    row = where_ref[0]
    if first:
        acc_ref[...] = jnp.zeros_like(acc_ref)
    for hop, own, other in pieces:
        block = hop % HALF
        head = lax.rem(row - hop + RING, RING) // HALF
        part = jnp.dot(x_ref[2 * block], own[...], preferred_element_type=jnp.float32)
        part += jnp.dot(x_ref[2 * block + 1], other[...], preferred_element_type=jnp.float32)
        acc_ref[pl.ds(head, 1)] += part[None]


def early_kernel(hops, where_ref, x_ref, *refs):
    *weights, acc_ref = refs
    pieces = [(hop, weights[2 * i], weights[2 * i + 1]) for i, hop in enumerate(hops)]
    project(where_ref, x_ref, acc_ref, pieces, True)


def late_kernel(hops, where_ref, x_ref, acc_in, q_ref, cos_ref, sin_ref, keep_ref, *refs):
    *weights, probs_ref, values_ref, acc_ref = refs
    acc_ref[...] = acc_in[...]
    pieces = [(hop, weights[2 * i], weights[2 * i + 1]) for i, hop in enumerate(hops)]
    project(where_ref, x_ref, acc_ref, pieces, False)

    @pl.when(where_ref[1] == 1)
    def _():
        cosine, sine = cos_ref[...], sin_ref[...]
        keep = keep_ref[...] > 0.0
        lane = lax.broadcasted_iota(jnp.int32, (keep.shape[0], 128), 1)
        for head in range(2):
            first, second = acc_ref[head, :, : HEAD // 2], acc_ref[head, :, HEAD // 2 :]
            keys = jnp.concatenate(
                [first * cosine - second * sine, second * cosine + first * sine], axis=1
            ).astype(jnp.bfloat16)
            score = lax.dot_general(
                q_ref[head], keys, (((1,), (1,)), ((), ())), preferred_element_type=jnp.float32
            ) * HEAD ** (-0.5)
            masked = jnp.where(keep, score, jnp.float32(-1e30))
            row_max = jnp.max(masked, axis=1, keepdims=True)
            probs = jnp.where(keep, jnp.exp(masked - row_max), jnp.float32(0.0))
            row_sum = jnp.sum(probs, axis=1, keepdims=True)
            probs_ref[head, :, :HEAD] = probs
            probs_ref[head, :, HEAD:] = jnp.where(lane % 64 < 32, row_max, row_sum)
        values_ref[...] = jnp.zeros_like(values_ref)

    @pl.when(where_ref[1] == 0)
    def _():
        values_ref[...] = acc_ref[...].astype(jnp.bfloat16)
        probs_ref[...] = jnp.zeros_like(probs_ref)


def weigh_kernel(where_ref, probs_ref, values_ref, out_ref):
    n_seqs = out_ref.shape[1]

    @pl.when(where_ref[1] == 0)
    def _():
        for head in range(2):
            half = values_ref.shape[1] // 2
            probs = jnp.concatenate([probs_ref[head, :, half : 2 * half], probs_ref[head, :, :half]], axis=1)
            values = values_ref[head]
            total = jnp.zeros((probs.shape[0], HEAD), jnp.float32)
            for _ in range(3):
                top = probs.astype(jnp.bfloat16)
                total += jnp.dot(top, values, preferred_element_type=jnp.float32)
                probs = probs - top.astype(jnp.float32)
            stats = probs_ref[head, :, HEAD + 64 : HEAD + 128]
            for target in range(HALF):
                query, col = target // 4, target % 4 * 64
                rows = slice(query * n_seqs, (query + 1) * n_seqs)
                out_ref[head * HALF + target] = jnp.concatenate(
                    [total[rows, col : col + 64], stats[rows]], axis=1
                )

    @pl.when(where_ref[1] == 1)
    def _():
        out_ref[...] = jnp.zeros_like(out_ref)


def merge_kernel(parts_ref, out_ref):
    n_parts = parts_ref.shape[0]
    tops = [parts_ref[i, :, 64:65] for i in range(n_parts)]
    top = functools.reduce(jnp.maximum, tops)
    total, weight = 0.0, 0.0
    for i in range(n_parts):
        scale = jnp.exp(tops[i] - top)
        total += scale * parts_ref[i, :, :64]
        weight += scale * parts_ref[i, :, 96:97]
    out_ref[...] = (total / weight).astype(jnp.bfloat16)


def shards(hidden, norm_gain, kv_weight, queries, page_seqs, page_slots, lengths):
    n_devices = lax.axis_size("seq")
    n_cols = n_devices // (RING * CORES)
    index = lax.axis_index("seq")
    core, row, col = index % CORES, index // CORES % RING, index // (RING * CORES)
    place = jnp.stack([row, core]).astype(jnp.int32)
    send = lambda array, step: lax.ppermute(array, "seq", moves(n_devices, step))
    up = lambda a: send(a, lambda x, z, c: (x, z + 1, c))
    down = lambda a: send(a, lambda x, z, c: (x, z - 1, c))
    right = lambda a: send(a, lambda x, z, c: (x + 1, z, c))
    left = lambda a: send(a, lambda x, z, c: (x - 1, z, c))
    across = lambda a: send(a, lambda x, z, c: (x, z, 1 - c))

    depth = kv_weight.shape[0]
    own = jnp.where(core == 1, kv_weight[:, :HEAD], kv_weight[:, HEAD:])
    other = across(jnp.where(core == 1, kv_weight[:, HEAD:], kv_weight[:, :HEAD]))
    weights = {0: (own, other)}
    for hop in range(1, HALF):
        weights[hop] = tuple(up(piece) for piece in weights[hop - 1])
        weights[-hop] = tuple(down(piece) for piece in weights[1 - hop])
    weights[HALF] = (up(weights[HALF - 1][0]), down(weights[1 - HALF][1]))

    n_tok, width = hidden.shape
    wide = hidden.astype(jnp.float32)
    scale_rows = lax.rsqrt(jnp.mean(wide * wide, axis=1, keepdims=True) + 1e-06)
    normed = (wide * scale_rows * (1.0 + norm_gain)[None, :]).astype(jnp.bfloat16)
    cut = normed.reshape(n_tok, HALF, CORES, depth).transpose(1, 2, 0, 3)[::-1]
    cut = lax.dynamic_slice_in_dim(jnp.concatenate([cut, cut]), (HALF - 1 - row) % HALF, HALF, 0)
    cut = jnp.where(core == 0, cut, cut[:, ::-1])
    from_left, from_right = right(cut), left(cut)
    opposite = jnp.concatenate([right(from_left[: HALF // 2]), left(from_right[HALF // 2 :])])
    mine = jnp.concatenate([cut, from_left, from_right, opposite], axis=2)
    theirs = across(mine)[:, ::-1]
    tokens = jnp.concatenate([mine, theirs], axis=2)
    n_held = tokens.shape[2]
    tokens = tokens.reshape(HALF * CORES, n_held, depth)

    page_dev = page_seqs.shape[0] // n_devices
    page_len = n_tok // page_dev
    cols = (col + jnp.array([0, -1, 1, 2], jnp.int32)) % n_cols
    holders = (cols[None, :] * RING + row) * CORES + jnp.stack([core, 1 - core])[:, None]
    page_ids = (holders[:, :, None] * page_dev + jnp.arange(page_dev, dtype=jnp.int32)).reshape(-1)
    seq_ids = jnp.repeat(page_seqs[page_ids], page_len)
    positions = (
        page_slots[page_ids][:, None] * page_len + jnp.arange(page_len, dtype=jnp.int32)[None, :]
    ).reshape(-1)
    half_dim = HEAD // 2
    inverse_freq = jnp.exp(
        -(2.0 * jnp.arange(half_dim, dtype=jnp.float32) / HEAD) * jnp.log(jnp.float32(10000.0))
    )
    angles = positions.astype(jnp.float32)[:, None] * inverse_freq[None, :]
    cosine, sine = jnp.cos(angles), jnp.sin(angles)
    n_seqs = queries.shape[0]
    keep = (seq_ids[None, :] == jnp.arange(n_seqs, dtype=jnp.int32)[:, None]) & (
        positions[None, :] < lengths[:, None]
    )
    keep = jnp.tile(keep.astype(jnp.float32), (2, 1))
    heads = lax.dynamic_slice_in_dim(queries, 4 * col, 4, 1)
    heads = heads.transpose(1, 0, 2).reshape(2, 2 * n_seqs, HEAD)

    early = [0] + [sign * hop for hop in range(1, 6) for sign in (1, -1)]
    late = [sign * hop for hop in range(6, HALF) for sign in (1, -1)] + [HALF]
    pieces = lambda hops: [piece for hop in hops for piece in weights[hop]]
    held = pl.pallas_call(
        functools.partial(early_kernel, early),
        out_shape=jax.ShapeDtypeStruct((2, n_held, HEAD), jnp.float32),
        in_specs=[SMEM] + [VMEM] * (1 + 2 * len(early)),
        out_specs=VMEM,
        name="early",
    )(place, tokens, *pieces(early))
    probs, values = pl.pallas_call(
        functools.partial(late_kernel, late),
        out_shape=(
            jax.ShapeDtypeStruct((2, 2 * n_seqs, HEAD + 128), jnp.float32),
            jax.ShapeDtypeStruct((2, n_held, HEAD), jnp.bfloat16),
        ),
        in_specs=[SMEM] + [VMEM] * (6 + 2 * len(late)),
        out_specs=(VMEM, VMEM),
        scratch_shapes=[pltpu.VMEM((2, n_held, HEAD), jnp.float32)],
        name="late",
    )(place, tokens, held, heads, cosine, sine, keep, *pieces(late))
    probs = lax.ppermute(probs, "seq", [(i + 1, i) for i in range(0, n_devices, CORES)])
    parts = pl.pallas_call(
        weigh_kernel,
        out_shape=jax.ShapeDtypeStruct((RING, n_seqs, 128), jnp.float32),
        in_specs=[SMEM, VMEM, VMEM],
        out_specs=VMEM,
        name="weigh",
    )(place, probs, values)
    rings = [
        [(x * RING + z) * CORES + c for z in range(RING)] for x in range(n_cols) for c in range(CORES)
    ]
    parts = lax.all_to_all(parts, "seq", 0, 0, axis_index_groups=rings, tiled=True)
    done = pl.pallas_call(
        merge_kernel,
        out_shape=jax.ShapeDtypeStruct((n_seqs, 64), jnp.bfloat16),
        in_specs=[VMEM],
        out_specs=VMEM,
        name="merge",
    )(parts)
    given = lax.ppermute(done[:, 32:], "seq", [(i, i + 1) for i in range(0, n_devices, CORES)])
    return jnp.where(core == 0, done[:, :32], given)


def solution(mesh):
    placed = (
        P(("groups", "seq"), None),
        P(),
        P("seq", None),
        P("groups", None, None),
        P("groups"),
        P("groups"),
        P("groups"),
    )
    return jax.shard_map(
        shards, mesh=mesh, in_specs=placed, out_specs=P("groups", "seq"), check_vma=False
    )
```

```python
import functools

import jax
import jax.numpy as jnp
from jax import lax
from jax.experimental import pallas as pl
from jax.experimental.pallas import tpu as pltpu
from jax.sharding import PartitionSpec as P

HEAD = 256
KVH = 8
CORES = 2
RING = 16
HALF = RING // 2
EARLY = 6


VMEM = pl.BlockSpec(memory_space=pltpu.VMEM)
SMEM = pl.BlockSpec(memory_space=pltpu.SMEM)


def moves(n_devices, step, cores=range(CORES)):
    n_cols = n_devices // (RING * CORES)
    pairs = []
    for i in range(n_devices):
        col, row, core = i // (RING * CORES), i // CORES % RING, i % CORES
        if core in cores:
            col, row, core = step(col, row, core)
            pairs.append((i, (col % n_cols * RING + row % RING) * CORES + core))
    return pairs


def split(value):
    top = value.astype(jnp.bfloat16)
    return jnp.concatenate([top, (value - top.astype(jnp.float32)).astype(jnp.bfloat16)], axis=0)


def norm_kernel(where_ref, hidden_ref, gain_ref, out_ref):
    row, core = where_ref[0], where_ref[1]
    depth = out_ref.shape[3]
    wide = hidden_ref[...].astype(jnp.float32)
    scale = lax.rsqrt(jnp.mean(wide * wide, axis=1, keepdims=True) + 1e-06)
    normed = (wide * scale * (1.0 + gain_ref[...])).astype(jnp.bfloat16)
    for block in range(HALF):
        ahead = lax.rem(row - block + RING, HALF)
        hop = jnp.where(core == 0, ahead, lax.rem(HALF - ahead, HALF))
        for half in range(CORES):
            at = (block * CORES + half) * depth
            out_ref[hop, half ^ core] = normed[:, at : at + depth]


def columns(token_refs, hop, half):
    n = len(token_refs) // 2
    own = [ref[hop % HALF, half] for ref in token_refs[:n]]
    far = [ref[-hop % HALF, 1 - half] for ref in token_refs[n:]]
    return jnp.concatenate(own + far, axis=0)


def head_of(where_ref, hop):
    shift = jnp.where(where_ref[1] == 0, RING - hop, hop)
    return lax.rem(where_ref[0] + shift, RING) // HALF


def project(where_ref, token_refs, weight_refs, hops, acc_ref):
    for i, hop in enumerate(hops):
        part = sum(
            jnp.dot(
                columns(token_refs, hop, half),
                weight_refs[2 * i + half][...],
                preferred_element_type=jnp.float32,
            )
            for half in range(CORES)
        )
        if hop == 0:
            part = jnp.where(where_ref[1] == 0, part, 0.0)
        acc_ref[pl.ds(head_of(where_ref, hop), 1)] += part[None]


def early_kernel(hops, n_pieces, where_ref, *refs):
    acc_ref = refs[-1]
    acc_ref[...] = jnp.zeros_like(acc_ref)
    project(where_ref, refs[:n_pieces], refs[n_pieces:-1], hops, acc_ref)


def late_kernel(hops, n_pieces, where_ref, held_ref, *refs):
    *refs, kept_ref, sent_ref, acc_ref = refs
    acc_ref[...] = held_ref[...]
    project(where_ref, refs[:n_pieces], refs[n_pieces:], hops, acc_ref)
    core = where_ref[1]
    kept_ref[...] = acc_ref[pl.ds(core, 1)][0]
    half = sent_ref.shape[0] // 2
    sent = acc_ref[pl.ds(1 - core, 1)][0]
    sent_ref[:half] = sent[half:]
    sent_ref[half:] = sent[:half]


def score_kernel(kept_ref, came_ref, q_ref, cos_ref, sin_ref, keep_ref, probs_ref):
    raw = kept_ref[...] + came_ref[...]
    cosine, sine = cos_ref[...], sin_ref[...]
    keep = keep_ref[...] > 0.0
    first, second = raw[:, : HEAD // 2], raw[:, HEAD // 2 :]
    keys = jnp.concatenate(
        [first * cosine - second * sine, second * cosine + first * sine], axis=1
    ).astype(jnp.bfloat16)
    score = lax.dot_general(
        q_ref[...], keys, (((1,), (1,)), ((), ())), preferred_element_type=jnp.float32
    ) * HEAD ** (-0.5)
    masked = jnp.where(keep, score, jnp.float32(-1e30))
    row_max = jnp.max(masked, axis=1, keepdims=True)
    probs = jnp.where(keep, jnp.exp(masked - row_max), jnp.float32(0.0))
    row_sum = jnp.sum(probs, axis=1, keepdims=True)
    lane = lax.broadcasted_iota(jnp.int32, (keep.shape[0], 128), 1)
    probs_ref[:, :HEAD] = probs
    probs_ref[:, HEAD:] = jnp.where(lane < 64, row_max, row_sum)


def mix_kernel(where_ref, own_ref, other_ref, *refs):
    *token_refs, out_ref = refs
    core = where_ref[1]
    own, other = own_ref[:, :HEAD], other_ref[:, :HEAD]
    half = HEAD // 2
    other = jnp.concatenate([other[:, half:], other[:, :half]], axis=1)
    n = own.shape[0]
    probs = jnp.concatenate([split(own), split(other)], axis=0)
    for hop in range(HALF):
        for part in range(CORES):
            both = jnp.dot(probs, columns(token_refs, hop, part), preferred_element_type=jnp.float32)
            out_ref[CORES * hop + part, pl.ds(core, 1)] = split(both[:n] + both[n : 2 * n])[None]
            out_ref[CORES * hop + part, pl.ds(1 - core, 1)] = split(both[2 * n : 3 * n] + both[3 * n :])[None]


def weigh_kernel(where_ref, mixed_ref, *refs):
    *weight_refs, out_ref, acc_ref = refs
    acc_ref[...] = jnp.zeros_like(acc_ref)
    for hop in range(HALF + 1):
        head = head_of(where_ref, hop)
        part = sum(
            jnp.dot(
                mixed_ref[CORES * (hop % HALF) + half, pl.ds(head, 1)][0],
                weight_refs[2 * hop + half][...],
                preferred_element_type=jnp.float32,
            )
            for half in range(CORES)
        )
        if hop == 0:
            part = jnp.where(where_ref[1] == 0, part, 0.0)
        acc_ref[pl.ds(head, 1)] += part[None]
    n = out_ref.shape[1]
    out_ref[...] = acc_ref[:, :n] + acc_ref[:, n:]


def deal_kernel(n_seqs, where_ref, own_ref, came_ref, own_probs_ref, other_probs_ref, out_ref):
    core = where_ref[1]
    lane = lax.broadcasted_iota(jnp.int32, (n_seqs, 128), 1)
    for head in range(2):
        total = own_ref[head] + came_ref[head]
        stats = jnp.where(core == head, own_probs_ref[:, HEAD:], other_probs_ref[:, HEAD:])
        for target in range(HALF):
            query, col = target // 4, target % 4 * 64
            rows = slice(query * n_seqs, (query + 1) * n_seqs)
            pair = total[rows, col : col + 64]
            mine = jnp.where(core == 0, pair[:, :32], pair[:, 32:])
            out_ref[head * HALF + target] = jnp.concatenate(
                [mine, stats[rows, 32:96], mine], axis=1
            )


def merge_kernel(parts_ref, out_ref):
    n_parts = parts_ref.shape[0]
    tops = [parts_ref[i, :, 32:33] for i in range(n_parts)]
    top = functools.reduce(jnp.maximum, tops)
    total, weight = 0.0, 0.0
    for i in range(n_parts):
        scale = jnp.exp(tops[i] - top)
        total += scale * parts_ref[i, :, :32]
        weight += scale * parts_ref[i, :, 64:65]
    out_ref[...] = (total / weight).astype(jnp.bfloat16)


def shards(hidden, norm_gain, kv_weight, queries, page_seqs, page_slots, lengths):
    n_devices = lax.axis_size("seq")
    n_cols = n_devices // (RING * CORES)
    index = lax.axis_index("seq")
    core, row, col = index % CORES, index // CORES % RING, index // (RING * CORES)
    place = jnp.stack([row, core]).astype(jnp.int32)
    depth = kv_weight.shape[0]
    n_seqs = queries.shape[0]
    n_tok, width = hidden.shape
    f32, bf16 = jnp.float32, jnp.bfloat16
    shape = jax.ShapeDtypeStruct

    around = moves(n_devices, lambda x, z, c: (x, z + 1 - 2 * c, c))
    last = moves(n_devices, lambda x, z, c: (x, z + 1 - 2 * c, c), (1,))
    beside = moves(n_devices, lambda x, z, c: (x + 1 - 2 * c, z, c))
    across = moves(n_devices, lambda x, z, c: (x, z, 1 - c))
    send = lambda array, pairs: lax.ppermute(array, "seq", pairs)

    keys, values = kv_weight[:, :HEAD], kv_weight[:, HEAD:]
    key_ring = [(keys, send(keys, across))]
    value_ring = [(values, send(values, across))]
    for hop in range(1, HALF + 1):
        pairs = around if hop < HALF else last
        key_ring.append(tuple(send(piece, pairs) for piece in key_ring[-1]))
        value_ring.append(tuple(send(piece, pairs) for piece in value_ring[-1]))

    normed = pl.pallas_call(
        norm_kernel,
        out_shape=shape((HALF, CORES, n_tok, depth), bf16),
        in_specs=[SMEM, VMEM, VMEM],
        out_specs=VMEM,
        name="norm",
    )(place, hidden, norm_gain[None, :])
    mine = [normed]
    for _ in range(n_cols - 1):
        mine.append(send(mine[-1], beside))
    tokens = mine + [send(piece, across) for piece in mine]
    n_held = n_tok * len(tokens)

    page_dev = page_seqs.shape[0] // n_devices
    page_len = n_tok // page_dev
    cores = jnp.stack([core, 1 - core])[:, None]
    cols = (col + (2 * cores - 1) * jnp.arange(n_cols, dtype=jnp.int32)) % n_cols
    holders = (cols * RING + row) * CORES + cores
    page_ids = (holders[:, :, None] * page_dev + jnp.arange(page_dev, dtype=jnp.int32)).reshape(-1)
    seq_ids = jnp.repeat(page_seqs[page_ids], page_len)
    positions = (
        page_slots[page_ids][:, None] * page_len + jnp.arange(page_len, dtype=jnp.int32)[None, :]
    ).reshape(-1)
    half_dim = HEAD // 2
    inverse_freq = jnp.exp(
        -(2.0 * jnp.arange(half_dim, dtype=jnp.float32) / HEAD) * jnp.log(jnp.float32(10000.0))
    )
    angles = positions.astype(jnp.float32)[:, None] * inverse_freq[None, :]
    cosine, sine = jnp.cos(angles), jnp.sin(angles)
    keep = (seq_ids[None, :] == jnp.arange(n_seqs, dtype=jnp.int32)[:, None]) & (
        positions[None, :] < lengths[:, None]
    )
    keep = jnp.tile(keep.astype(jnp.float32), (2, 1))
    head = lax.dynamic_slice_in_dim(queries, 4 * col + 2 * core, 2, 1)
    head = head.transpose(1, 0, 2).reshape(2 * n_seqs, HEAD)

    flat = lambda steps: [piece for step in steps for piece in step]
    early, late = range(EARLY), range(EARLY, HALF + 1)
    held = pl.pallas_call(
        functools.partial(early_kernel, early, len(tokens)),
        out_shape=shape((2, n_held, HEAD), f32),
        in_specs=[SMEM] + [VMEM] * (len(tokens) + 2 * len(early)),
        out_specs=VMEM,
        name="early",
    )(place, *tokens, *flat(key_ring[:EARLY]))
    kept, sent = pl.pallas_call(
        functools.partial(late_kernel, late, len(tokens)),
        out_shape=(shape((n_held, HEAD), f32), shape((n_held, HEAD), f32)),
        in_specs=[SMEM] + [VMEM] * (1 + len(tokens) + 2 * len(late)),
        out_specs=(VMEM, VMEM),
        scratch_shapes=[pltpu.VMEM((2, n_held, HEAD), f32)],
        name="late",
    )(place, held, *tokens, *flat(key_ring[EARLY:]))
    came = send(sent, across)
    probs = pl.pallas_call(
        score_kernel,
        out_shape=shape((2 * n_seqs, HEAD + 128), f32),
        in_specs=[VMEM] * 6,
        out_specs=VMEM,
        name="score",
    )(kept, came, head, cosine, sine, keep)
    other_probs = send(probs, across)
    mixed = pl.pallas_call(
        mix_kernel,
        out_shape=shape((HALF * CORES, 2, 4 * n_seqs, depth), bf16),
        in_specs=[SMEM] + [VMEM] * (2 + len(tokens)),
        out_specs=VMEM,
        name="mix",
    )(place, probs, other_probs, *tokens)
    weighed = pl.pallas_call(
        weigh_kernel,
        out_shape=shape((2, 2 * n_seqs, HEAD), f32),
        in_specs=[SMEM] + [VMEM] * (1 + 2 * len(value_ring)),
        out_specs=VMEM,
        scratch_shapes=[pltpu.VMEM((2, 4 * n_seqs, HEAD), f32)],
        name="weigh",
    )(place, mixed, *flat(value_ring))
    parts = pl.pallas_call(
        functools.partial(deal_kernel, n_seqs),
        out_shape=shape((RING, n_seqs, 128), f32),
        in_specs=[SMEM] + [VMEM] * 4,
        out_specs=VMEM,
        name="deal",
    )(place, weighed, send(weighed, across), probs, other_probs)
    rings = [
        [(x * RING + z) * CORES + c for z in range(RING)] for x in range(n_cols) for c in range(CORES)
    ]
    parts = lax.all_to_all(parts, "seq", 0, 0, axis_index_groups=rings, tiled=True)
    return pl.pallas_call(
        merge_kernel,
        out_shape=shape((n_seqs, HEAD // 8), bf16),
        in_specs=[VMEM],
        out_specs=VMEM,
        name="merge",
    )(parts)


def solution(mesh):
    placed = (
        P(("groups", "seq"), None),
        P(),
        P("seq", None),
        P("groups", None, None),
        P("groups"),
        P("groups"),
        P("groups"),
    )
    return jax.shard_map(
        shards, mesh=mesh, in_specs=placed, out_specs=P("groups", "seq"), check_vma=False
    )
```
